128 devices in a mesh: ep: 8 (over x, core), fsdp: 16 (over z, y).
Axes of the slice: x: 4, y: 4, z: 4, core: 2. Of those that a mesh axis runs over, the one named last changes fastest.
Arguments:
- master_gate: float32 [128, 2048, 768], P('ep', 'fsdp'), may hold values from -0.1875 to 0.1875
- master_up: float32 [128, 2048, 768], P('ep', 'fsdp'), may hold values from -0.1875 to 0.1875
- router_weight: float32 [2048, 128], P('fsdp', 'ep'), may hold values from -0.125 to 0.125
- router_gain: float32 [2048], P('fsdp'), may hold values from 0.25 to 1.75
Outputs:
- final_gate: bfloat16 [128, 2048, 768], P(('ep', 'fsdp'))
- final_up: bfloat16 [128, 2048, 768], P(('ep', 'fsdp'))
- scale_gate: float32 [128, 768], P(('ep', 'fsdp'))
- scale_up: float32 [128, 768], P(('ep', 'fsdp'))
- serve_router: bfloat16 [2048, 128], replicated
The draws below stay inside these ranges and needn't reach their ends.
All inputs are finite; a program needn't handle non-finite values.
Results may differ from the reference program's by a relative error of at most 0.001.
Values may be sent and summed in bfloat16 or wider, within the bound.
A program may use at most 128 MiB of HBM per device.

```python
import jax
import jax.numpy as jnp
from jax import lax

EXPERTS = 128
D_MODEL = 2048
D_EXPERT = 768


def with_spikes(drawn, own_key, source, target, blocks, factor):
    owner, partner = [(jnp.arange(drawn.shape[axis_at]) // (drawn.shape[axis_at] // blocks)).reshape([-1 if axis == axis_at else 1 for axis in range(drawn.ndim)]) for axis_at in (source, target)]
    chosen = jax.random.permutation(own_key, blocks)[partner]
    strong = (owner == chosen) | (owner == (partner + blocks // 2) % blocks)
    return jnp.where(strong, factor * drawn, drawn)


def level_of(stream_key, dims, pieces, least, high):
    loudness = 1.0
    for dim, parts in pieces:
        heights = jax.random.uniform(jax.random.fold_in(jax.random.fold_in(stream_key, 6), dim), (parts,), jnp.float32, least / len(pieces), high / len(pieces))
        loudness = loudness * jnp.repeat(jnp.exp(heights), dims[dim] // parts).reshape((-1,) + (1,) * (len(dims) - 1 - dim))
    return loudness


def noise(rng, shape, scale, limit, pieces=(), kind=jnp.bfloat16):
    result = scale * jax.random.normal(rng, shape, jnp.float32)
    if pieces:
        result = result * level_of(rng, shape, pieces, -0.22, 0.18)
    return jnp.clip(result, -limit, limit).astype(kind)


def gaussian_with(stream_key, extent, spread, most, cuts, heavy, kind=jnp.bfloat16):
    result = spread * jax.random.normal(stream_key, extent, jnp.float32)
    if cuts:
        result = result * level_of(stream_key, extent, cuts, -0.22, 0.18)
    return jnp.clip(with_spikes(result, jax.random.fold_in(stream_key, 3), *heavy), -most, most).astype(kind)


def setup_inputs(seed: int = 0) -> dict:
    streams_of = jax.random.split(jax.random.key(seed), 5)
    return {
        "master_gate": gaussian_with(streams_of[0], (EXPERTS, D_MODEL, D_EXPERT), D_MODEL ** -0.5, 0.1875, ((0, 8), (1, 16)), (1, 2, 16, 2.0), jnp.float32),
        "master_up": gaussian_with(streams_of[1], (EXPERTS, D_MODEL, D_EXPERT), D_MODEL ** -0.5, 0.1875, ((0, 8), (1, 16)), (1, 2, 16, 2.0), jnp.float32),
        "router_weight": noise(streams_of[2], (D_MODEL, EXPERTS), D_MODEL ** -0.5, 0.125, ((0, 16), (1, 8)), jnp.float32),
        "router_gain": jnp.clip(1.0 + 0.15 * jax.random.normal(streams_of[3], (D_MODEL,), jnp.float32), 0.25, 1.75),
    }


def reference(master_gate, master_up, router_weight, router_gain):
    scale_gate = jnp.sqrt(lax.optimization_barrier(jnp.sum(master_gate * master_gate, axis=1)))
    final_gate = (master_gate / jnp.expand_dims(scale_gate, 1)).astype(jnp.bfloat16)
    scale_up = jnp.sqrt(lax.optimization_barrier(jnp.sum(master_up * master_up, axis=1)))
    final_up = (master_up / jnp.expand_dims(scale_up, 1)).astype(jnp.bfloat16)
    serve_router = (router_weight * router_gain[:, None]).astype(jnp.bfloat16)
    return (final_gate, final_up, scale_gate, scale_up, serve_router)
```

```python
import functools

import jax
import jax.numpy as jnp
from jax import lax
from jax.experimental import pallas as pl
from jax.experimental.pallas import tpu as pltpu
from jax.sharding import PartitionSpec as P

MESH = pl.DeviceIdType.MESH
LANES = 128
ORDER = (
    (2, 2), (2, 1), (1, 2), (2, 3), (3, 2), (1, 1), (3, 3), (1, 3),
    (3, 1), (2, 0), (0, 2), (1, 0), (0, 1), (3, 0), (0, 3),
)


def kernel(
    ep_size, side, gate, up, weight, gain,
    final_gate, final_up, scale_gate, scale_up, router,
    x, sums, first, firsts, parts, totals, inverse, sent, rows, columns,
    in_sem, small_sem, first_sem, part_sem, total_sem, row_sem, column_sem, block_sem, own_sem,
):
    fsdp = side * side
    experts, depth = gate.shape[0], gate.shape[1]
    groups = gate.shape[2] // LANES
    chunks = 2 * groups
    ep, me = lax.axis_index("ep"), lax.axis_index("fsdp")
    my_z, my_y = me // side, me % side
    order = [((my_z + dz) % side) * side + (my_y + dy) % side for dy, dz in ORDER]
    others = [(ep + step) % ep_size for step in range(1, ep_size)]

    barrier = pltpu.get_barrier_semaphore()
    for peer in order:
        pl.semaphore_signal(barrier, inc=1, device_id=(ep, peer), device_id_type=MESH)
    for other in others:
        pl.semaphore_signal(barrier, inc=1, device_id=(other, me), device_id_type=MESH)

    def read(chunk):
        source = gate if chunk < groups else up
        at = (chunk % groups) * LANES
        return pltpu.make_async_copy(
            source.at[:, :, pl.ds(at, LANES)], x.at[chunk], in_sem.at[chunk]
        )

    for chunk in range(chunks):
        read(chunk).start()

    def remote(source, target, sems, device):
        return pltpu.make_async_remote_copy(
            src_ref=source, dst_ref=target, send_sem=sems.at[0], recv_sem=sems.at[1],
            device_id=device, device_id_type=MESH,
        )

    def square_sum(chunk, e):
        block = x[chunk, e]
        return jnp.sum(block * block, axis=0, keepdims=True)

    rows[me] = (weight[...] * gain[...]).astype(jnp.bfloat16)

    read(0).wait()
    for e in range(experts):
        total = square_sum(0, e)
        first[pl.ds(e, 1), :] = total
        sums[e, pl.ds(0, 1), :] = total
    pl.semaphore_wait(barrier, len(order) + len(others))
    for peer in order:
        remote(first, firsts.at[me], first_sem, (ep, peer)).start()
    for peer in order:
        remote(rows.at[me], rows.at[me], row_sem, (ep, peer)).start()
    firsts[me] = first[...]

    for chunk in range(1, chunks):
        read(chunk).wait()

    def sum_chunk(chunk, carry):
        for e in range(experts):
            sums[e, pl.ds(chunk, 1), :] = square_sum(chunk, e)
        return carry

    lax.fori_loop(1, chunks, sum_chunk, 0)
    for peer in order:
        remote(sums.at[peer], parts.at[me], part_sem, (ep, peer)).start()
    parts[me] = sums[me]

    def all_of(ref, sem):
        pltpu.make_async_copy(ref, ref, sem).wait()

    def send_chunk(target, chunk, at, scaled):
        columns_at = pl.ds(at, LANES)
        waiting = None
        for peer in order + [me]:
            block = x[chunk, peer] * scaled(peer)
            sent[chunk, peer] = block.astype(jnp.bfloat16)
            if waiting is not None:
                remote(
                    sent.at[chunk, waiting], target.at[pl.ds(me * depth, depth), columns_at],
                    block_sem, (ep, waiting),
                ).start()
            waiting = peer
        pltpu.make_async_copy(
            sent.at[chunk, me], target.at[pl.ds(me * depth, depth), columns_at], own_sem
        ).start()

    all_of(firsts.at[pl.ds(0, fsdp - 1)], first_sem.at[1])
    total = firsts[0]
    for s in range(1, fsdp):
        total = total + firsts[s]
    first_inverse = 1.0 / jnp.sqrt(total)
    for e in range(experts):
        inverse[e, pl.ds(0, 1), :] = first_inverse[e : e + 1, :]
    send_chunk(final_gate, 0, 0, lambda e: inverse[e, pl.ds(0, 1), :])

    all_of(parts.at[pl.ds(0, fsdp - 1)], part_sem.at[1])
    total = parts[0]
    for s in range(1, fsdp):
        total = total + parts[s]
    totals[me] = total
    scale = jnp.sqrt(total)
    for j in range(groups):
        scale_gate[:, j * LANES : (j + 1) * LANES] = scale[j : j + 1, :]
        scale_up[:, j * LANES : (j + 1) * LANES] = scale[groups + j : groups + j + 1, :]
    for peer in order:
        remote(totals.at[me], totals.at[me], total_sem, (ep, peer)).start()

    all_of(rows.at[pl.ds(0, fsdp - 1)], row_sem.at[1])
    for other in others:
        remote(rows, columns.at[ep], column_sem, (other, me)).start()
    pltpu.make_async_copy(rows, columns.at[ep], small_sem).start()

    all_of(totals.at[pl.ds(0, fsdp - 1)], total_sem.at[1])

    def invert(e, carry):
        inverse[e] = 1.0 / jnp.sqrt(totals[e])
        return carry

    lax.fori_loop(0, experts, invert, 0)

    for half, target in enumerate((final_gate, final_up)):

        def send(j, carry, half=half, target=target):
            chunk = half * groups + j
            send_chunk(
                target, chunk, pl.multiple_of(j * LANES, LANES),
                lambda e: inverse[e, pl.ds(chunk, 1), :],
            )
            return carry

        lax.fori_loop(1 - half, groups, send, 0)

    pltpu.make_async_copy(rows, columns.at[ep], small_sem).wait()
    if others:
        all_of(columns.at[pl.ds(0, ep_size - 1)], column_sem.at[1])

    def turn(f, carry):
        block = columns[:, f].astype(jnp.float32).reshape(-1, depth)
        router[pl.ds(pl.multiple_of(f * depth, depth), depth), :] = block.T.astype(jnp.bfloat16)
        return carry

    lax.fori_loop(0, fsdp, turn, 0)

    all_of(firsts.at[pl.ds(0, fsdp - 1)], first_sem.at[0])
    all_of(parts.at[pl.ds(0, fsdp - 1)], part_sem.at[0])
    all_of(totals.at[pl.ds(0, fsdp - 1)], total_sem.at[0])
    all_of(rows.at[pl.ds(0, fsdp - 1)], row_sem.at[0])
    if others:
        all_of(columns.at[pl.ds(0, ep_size - 1)], column_sem.at[0])
    all_of(sent.at[:, 0], own_sem)
    all_of(sent.at[:, pl.ds(0, fsdp - 1)], block_sem.at[0])
    all_of(sent.at[:, pl.ds(0, fsdp - 1)], block_sem.at[1])


def body(ep_size, fsdp, master_gate, master_up, router_weight, router_gain):
    experts, depth, width = master_gate.shape
    side = 4
    own, columns = router_weight.shape[1], 2 * width // LANES
    anywhere = pl.BlockSpec(memory_space=pl.ANY)
    vmem = pl.BlockSpec(memory_space=pltpu.VMEM)
    dma, pair = pltpu.SemaphoreType.DMA, pltpu.SemaphoreType.DMA((2,))
    gate, up, scale_gate, scale_up, router = pl.pallas_call(
        functools.partial(kernel, ep_size, side),
        out_shape=(
            pltpu.VMEM((fsdp * depth, width), jnp.bfloat16),
            pltpu.VMEM((fsdp * depth, width), jnp.bfloat16),
            pltpu.VMEM((1, width), jnp.float32),
            pltpu.VMEM((1, width), jnp.float32),
            pltpu.VMEM((fsdp * depth, ep_size * own), jnp.bfloat16),
        ),
        in_specs=[anywhere, anywhere, vmem, vmem],
        out_specs=[vmem] * 5,
        scratch_shapes=[
            pltpu.VMEM((columns, experts, depth, LANES), jnp.float32),
            pltpu.VMEM((experts, columns, LANES), jnp.float32),
            pltpu.VMEM((experts, LANES), jnp.float32),
            pltpu.VMEM((fsdp, experts, LANES), jnp.float32),
            pltpu.VMEM((fsdp, columns, LANES), jnp.float32),
            pltpu.VMEM((fsdp, columns, LANES), jnp.float32),
            pltpu.VMEM((experts, columns, LANES), jnp.float32),
            pltpu.VMEM((columns, experts, depth, LANES), jnp.bfloat16),
            pltpu.VMEM((fsdp, own, depth), jnp.bfloat16),
            pltpu.VMEM((ep_size, fsdp, own, depth), jnp.bfloat16),
            dma((columns,)), dma,
            pair, pair, pair, pair, pair, pair, dma,
        ],
        compiler_params=pltpu.CompilerParams(
            collective_id=0, has_side_effects=True, vmem_limit_bytes=48 * 2**20
        ),
        name="relayout",
    )(master_gate, master_up, router_weight.T, router_gain[None, :])
    return gate[None], up[None], scale_gate, scale_up, router


def solution(mesh):
    both = ("ep", "fsdp")
    return jax.shard_map(
        functools.partial(body, mesh.shape["ep"], mesh.shape["fsdp"]),
        mesh=mesh,
        in_specs=(P("ep", "fsdp", None), P("ep", "fsdp", None), P("fsdp", "ep"), P("fsdp")),
        out_specs=(P(both, None, None), P(both, None, None), P(both, None), P(both, None), P()),
        check_vma=False,
    )
```

```python
import functools

import jax
import jax.numpy as jnp
from jax import lax
from jax.experimental import pallas as pl
from jax.experimental.pallas import tpu as pltpu
from jax.sharding import PartitionSpec as P

MESH = pl.DeviceIdType.MESH
LANES = 128
HEAD = 5
ORDER = (
    (2, 2), (2, 1), (1, 2), (2, 3), (3, 2), (1, 1), (3, 3), (1, 3),
    (3, 1), (2, 0), (0, 2), (1, 0), (0, 1), (3, 0), (0, 3),
)


def kernel(
    ep_size, side, stages, gate, up, weight, gain,
    final_gate, final_up, scale_gate, scale_up, router,
    x, sums, parts, totals, inverse, sent, rows, columns,
    in_sem, small_sem, part_sem, total_sem, row_sem, column_sem, block_sem, own_sem,
):
    fsdp = side * side
    experts, depth = gate.shape[0], gate.shape[1]
    groups = gate.shape[2] // LANES
    chunks = 2 * groups
    ep, me = lax.axis_index("ep"), lax.axis_index("fsdp")
    my_z, my_y = me // side, me % side
    order = [((my_z + dz) % side) * side + (my_y + dy) % side for dy, dz in ORDER]
    others = [(ep + step) % ep_size for step in range(1, ep_size)]
    scales = (scale_gate, scale_up)

    barrier = pltpu.get_barrier_semaphore()
    for peer in order:
        pl.semaphore_signal(barrier, inc=1, device_id=(ep, peer), device_id_type=MESH)
    for other in others:
        pl.semaphore_signal(barrier, inc=1, device_id=(other, me), device_id_type=MESH)

    def read(chunk):
        source = gate if chunk < groups else up
        at = (chunk % groups) * LANES
        return pltpu.make_async_copy(
            source.at[:, :, pl.ds(at, LANES)], x.at[chunk], in_sem.at[chunk]
        )

    for chunk in range(chunks):
        read(chunk).start()

    def remote(source, target, sems, device):
        return pltpu.make_async_remote_copy(
            src_ref=source, dst_ref=target, send_sem=sems.at[0], recv_sem=sems.at[1],
            device_id=device, device_id_type=MESH,
        )

    def all_of(ref, sem):
        pltpu.make_async_copy(ref, ref, sem).wait()

    def square_sum(chunk, e):
        block = x[chunk, e]
        return jnp.sum(block * block, axis=0, keepdims=True)

    def take_sums(stage):
        start, stop = stages[stage]
        for chunk in range(start, stop):
            read(chunk).wait()

        def one(chunk, carry):
            for e in range(experts):
                sums[stage][e, pl.ds(chunk - start, 1), :] = square_sum(chunk, e)
            return carry

        lax.fori_loop(start, stop, one, 0)

    def send_sums(stage):
        for peer in order:
            remote(sums[stage].at[peer], parts[stage].at[me], part_sem.at[stage], (ep, peer)).start()
        parts[stage][me] = sums[stage][me]

    def send_totals(stage):
        start, stop = stages[stage]
        all_of(parts[stage].at[pl.ds(0, fsdp - 1)], part_sem.at[stage, 1])
        total = parts[stage][0]
        for s in range(1, fsdp):
            total = total + parts[stage][s]
        totals[stage][me] = total
        scale = jnp.sqrt(total)
        for peer in order:
            remote(totals[stage].at[me], totals[stage].at[me], total_sem.at[stage], (ep, peer)).start()
        for chunk in range(start, stop):
            at = (chunk % groups) * LANES
            scales[chunk // groups][:, at : at + LANES] = scale[chunk - start : chunk - start + 1, :]

    def take_totals(stage):
        all_of(totals[stage].at[pl.ds(0, fsdp - 1)], total_sem.at[stage, 1])

        def invert(e, carry):
            inverse[stage][e] = 1.0 / jnp.sqrt(totals[stage][e])
            return carry

        lax.fori_loop(0, experts, invert, 0)

    def send_blocks(target, chunk, at, peers, scaled):
        place = (pl.ds(me * depth, depth), pl.ds(at, LANES))
        waiting = None
        for peer in peers + [None]:
            if peer is not None:
                sent[chunk, peer] = (x[chunk, peer] * scaled(peer)).astype(jnp.bfloat16)
            if waiting is not None:
                remote(sent.at[chunk, waiting], target.at[place], block_sem, (ep, waiting)).start()
            waiting = peer

    def keep_block(target, chunk, at, scaled):
        sent[chunk, me] = (x[chunk, me] * scaled(me)).astype(jnp.bfloat16)
        place = (pl.ds(me * depth, depth), pl.ds(at, LANES))
        pltpu.make_async_copy(sent.at[chunk, me], target.at[place], own_sem).start()

    def send_stage(stage):
        for half, target in enumerate((final_gate, final_up)):
            start = max(stages[stage][0], half * groups)
            stop = min(stages[stage][1], half * groups + groups)

            def send(chunk, carry, half=half, target=target):
                at = pl.multiple_of((chunk - half * groups) * LANES, LANES)
                scaled = lambda e: inverse[stage][e, pl.ds(chunk - stages[stage][0], 1), :]
                send_blocks(target, chunk, at, order, scaled)
                keep_block(target, chunk, at, scaled)
                return carry

            if start < stop:
                lax.fori_loop(start, stop, send, 0)

    rows[me] = (weight[...] * gain[...]).astype(jnp.bfloat16)

    read(0).wait()
    for e in range(experts):
        sums[0][pl.ds(e, 1), :] = square_sum(0, e)
    pl.semaphore_wait(barrier, len(order) + len(others))
    for peer in order:
        remote(sums[0], parts[0].at[me], part_sem.at[0], (ep, peer)).start()
    for peer in order:
        remote(rows.at[me], rows.at[me], row_sem, (ep, peer)).start()
    parts[0][me] = sums[0][...]

    for stage in range(1, len(stages)):
        take_sums(stage)
        send_sums(stage)

    all_of(parts[0].at[pl.ds(0, fsdp - 1)], part_sem.at[0, 1])
    total = parts[0][0]
    for s in range(1, fsdp):
        total = total + parts[0][s]
    totals[0][...] = total
    inverse[0][...] = 1.0 / jnp.sqrt(total)
    scale_gate[:, :LANES] = jnp.sqrt(totals[0][pl.ds(me, 1), :])
    scaled = lambda e: inverse[0][pl.ds(e, 1), :]

    send_blocks(final_gate, 0, 0, order[:HEAD], scaled)
    send_totals(1)
    send_blocks(final_gate, 0, 0, order[HEAD:], scaled)
    keep_block(final_gate, 0, 0, scaled)
    for stage in range(2, len(stages)):
        send_totals(stage)

    all_of(rows.at[pl.ds(0, fsdp - 1)], row_sem.at[1])
    for other in others:
        remote(rows, columns.at[ep], column_sem, (other, me)).start()
    pltpu.make_async_copy(rows, columns.at[ep], small_sem).start()

    for stage in range(1, len(stages)):
        take_totals(stage)
        send_stage(stage)

    pltpu.make_async_copy(rows, columns.at[ep], small_sem).wait()
    if others:
        all_of(columns.at[pl.ds(0, ep_size - 1)], column_sem.at[1])

    def turn(f, carry):
        block = columns[:, f].astype(jnp.float32).reshape(-1, depth)
        router[pl.ds(pl.multiple_of(f * depth, depth), depth), :] = block.T.astype(jnp.bfloat16)
        return carry

    lax.fori_loop(0, fsdp, turn, 0)

    for stage in range(len(stages)):
        all_of(parts[stage].at[pl.ds(0, fsdp - 1)], part_sem.at[stage, 0])
        if stage > 0:
            all_of(totals[stage].at[pl.ds(0, fsdp - 1)], total_sem.at[stage, 0])
    all_of(rows.at[pl.ds(0, fsdp - 1)], row_sem.at[0])
    if others:
        all_of(columns.at[pl.ds(0, ep_size - 1)], column_sem.at[0])
    all_of(sent.at[:, 0], own_sem)
    all_of(sent.at[:, pl.ds(0, fsdp - 1)], block_sem.at[0])
    all_of(sent.at[:, pl.ds(0, fsdp - 1)], block_sem.at[1])


def place(*refs):
    count = (len(refs) - 1) // 2
    copies = []
    for source, target in zip(refs[:count], refs[count : 2 * count]):
        pieces = 4 if source.shape[0] > 8 else 1
        step = source.shape[0] // pieces
        for k in range(pieces):
            at = pl.ds(k * step, step)
            copies.append(pltpu.make_async_copy(source.at[at], target.at[at], refs[-1].at[len(copies)]))
    for copy in copies:
        copy.start()
    for copy in copies:
        copy.wait()


def body(ep_size, fsdp, master_gate, master_up, router_weight, router_gain):
    experts, depth, width = master_gate.shape
    side = 4
    own, chunks = router_weight.shape[1], 2 * width // LANES
    stages = ((0, 1), (1, 4), (4, chunks))
    anywhere = pl.BlockSpec(memory_space=pl.ANY)
    vmem = pl.BlockSpec(memory_space=pltpu.VMEM)
    dma, pair = pltpu.SemaphoreType.DMA, pltpu.SemaphoreType.DMA((2,))

    def per_stage(lead, dtype=jnp.float32):
        return [pltpu.VMEM((lead, stop - start, LANES), dtype) for start, stop in stages[1:]]

    results = (
        ((fsdp * depth, width), jnp.bfloat16),
        ((fsdp * depth, width), jnp.bfloat16),
        ((1, width), jnp.float32),
        ((1, width), jnp.float32),
        ((fsdp * depth, ep_size * own), jnp.bfloat16),
    )
    flat = pltpu.VMEM((experts, LANES), jnp.float32)
    arrived = pl.pallas_call(
        functools.partial(kernel, ep_size, side, stages),
        out_shape=tuple(pltpu.VMEM(*result) for result in results),
        in_specs=[anywhere, anywhere, vmem, vmem],
        out_specs=[vmem] * 5,
        scratch_shapes=[
            pltpu.VMEM((chunks, experts, depth, LANES), jnp.float32),
            [flat] + per_stage(experts),
            [pltpu.VMEM((fsdp, experts, LANES), jnp.float32)] + per_stage(fsdp),
            [flat] + per_stage(experts),
            [flat] + per_stage(experts),
            pltpu.VMEM((chunks, experts, depth, LANES), jnp.bfloat16),
            pltpu.VMEM((fsdp, own, depth), jnp.bfloat16),
            pltpu.VMEM((ep_size, fsdp, own, depth), jnp.bfloat16),
            dma((chunks,)), dma, dma((len(stages), 2)), dma((len(stages), 2)),
            pair, pair, pair, dma,
        ],
        compiler_params=pltpu.CompilerParams(
            collective_id=0, has_side_effects=True, vmem_limit_bytes=48 * 2**20
        ),
        name="relayout",
    )(master_gate, master_up, router_weight.T, router_gain[None, :])
    gate, up, scale_gate, scale_up, router = pl.pallas_call(
        place,
        out_shape=tuple(jax.ShapeDtypeStruct(*result) for result in results),
        in_specs=[vmem] * 5,
        out_specs=[anywhere] * 5,
        scratch_shapes=[dma((16,))],
        compiler_params=pltpu.CompilerParams(vmem_limit_bytes=2**20),
        name="place",
    )(*(pltpu.with_memory_space_constraint(a, pltpu.VMEM) for a in arrived))
    return gate[None], up[None], scale_gate, scale_up, router


def solution(mesh):
    both = ("ep", "fsdp")
    return jax.shard_map(
        functools.partial(body, mesh.shape["ep"], mesh.shape["fsdp"]),
        mesh=mesh,
        in_specs=(P("ep", "fsdp", None), P("ep", "fsdp", None), P("fsdp", "ep"), P("fsdp")),
        out_specs=(P(both, None, None), P(both, None, None), P(both, None), P(both, None), P()),
        check_vma=False,
    )
```

```python
import functools

import jax
import jax.numpy as jnp
from jax import lax
from jax.experimental import pallas as pl
from jax.experimental.pallas import tpu as pltpu
from jax.sharding import PartitionSpec as P

MESH = pl.DeviceIdType.MESH
LANES = 128
HEAD = 0
RAW = 16
PIECE = 4
ORDER = (
    (2, 2), (2, 1), (1, 2), (2, 3), (3, 2), (1, 1), (3, 3), (1, 3),
    (3, 1), (2, 0), (0, 2), (1, 0), (0, 1), (3, 0), (0, 3),
)


def kernel(
    ep_size, side, stages, gate, up, weight, gain,
    final_gate, final_up, scale_gate, scale_up, router,
    x, sums, parts, totals, inverse, sent, raw, mine, rows, columns,
    in_sem, small_sem, part_sem, total_sem, raw_sem, row_sem, column_sem, block_sem, last_sem, own_sem, ready_sem,
):
    fsdp = side * side
    experts, depth = gate.shape[0], gate.shape[1]
    groups = gate.shape[2] // LANES
    chunks = 2 * groups
    ep, me = lax.axis_index("ep"), lax.axis_index("fsdp")
    my_z, my_y = me // side, me % side
    order = [((my_z + dz) % side) * side + (my_y + dy) % side for dy, dz in ORDER]
    others = [(ep + step) % ep_size for step in range(1, ep_size)]
    scales = (scale_gate, scale_up)
    last, short = (groups - 1) * LANES, depth - RAW

    barrier = pltpu.get_barrier_semaphore()
    reads = []
    for half, source in enumerate((gate, up)):
        for start, stop in ((0, 1), (1, 4), (4, groups)) if half == 0 else ((0, groups),):
            for e in range(0, experts, PIECE):
                part = (pl.ds(e, PIECE), slice(None), pl.ds(start * LANES, (stop - start) * LANES))
                copy = pltpu.make_async_copy(
                    source.at[part], x.at[(half, *part)], in_sem.at[len(reads)]
                )
                reads.append((half * groups + start, copy))
    for chunk, copy in reads:
        if chunk == 0:
            copy.start()
    for peer in order:
        pl.semaphore_signal(barrier, inc=1, device_id=(ep, peer), device_id_type=MESH)
    for other in others:
        @pl.when(other > ep)
        def _(other=other):
            pl.semaphore_signal(barrier, inc=1, device_id=(other, me), device_id_type=MESH)

    for chunk, copy in reads:
        if chunk > 0:
            copy.start()

    def wait_reads(start, stop):
        for chunk, copy in reads:
            if start <= chunk < stop:
                copy.wait()

    def block_of(chunk, e):
        half = chunk // groups
        return x[half, e, :, pl.ds(pl.multiple_of((chunk - half * groups) * LANES, LANES), LANES)]

    def remote(source, target, sems, device):
        return pltpu.make_async_remote_copy(
            src_ref=source, dst_ref=target, send_sem=sems.at[0], recv_sem=sems.at[1],
            device_id=device, device_id_type=MESH,
        )

    def all_of(ref, sem):
        pltpu.make_async_copy(ref, ref, sem).wait()

    def square_sum(chunk, e):
        block = block_of(chunk, e)
        return jnp.sum(block * block, axis=0, keepdims=True)

    def take_sums(stage):
        start, stop = stages[stage]
        wait_reads(start, stop)

        def one(chunk, carry):
            for e in range(experts):
                sums[stage][e, pl.ds(chunk - start, 1), :] = square_sum(chunk, e)
            return carry

        lax.fori_loop(start, stop, one, 0)

    def send_sums(stage):
        for peer in order:
            remote(sums[stage].at[peer], parts[stage].at[me], part_sem.at[stage], (ep, peer)).start()
        parts[stage][me] = sums[stage][me]

    def send_totals(stage):
        start, stop = stages[stage]
        all_of(parts[stage].at[pl.ds(0, fsdp - 1)], part_sem.at[stage, 1])
        total = parts[stage][0]
        for s in range(1, fsdp):
            total = total + parts[stage][s]
        totals[stage][me] = total
        if stop == chunks:
            mine[...] = 1.0 / jnp.sqrt(total)
        scale = jnp.sqrt(total)
        for peer in order:
            remote(totals[stage].at[me], totals[stage].at[me], total_sem.at[stage], (ep, peer)).start()
        for chunk in range(start, stop):
            at = (chunk % groups) * LANES
            scales[chunk // groups][:, at : at + LANES] = scale[chunk - start : chunk - start + 1, :]

    def take_totals(stage):
        all_of(totals[stage].at[pl.ds(0, fsdp - 1)], total_sem.at[stage, 1])

        def invert(e, carry):
            inverse[stage][e] = 1.0 / jnp.sqrt(totals[stage][e])
            return carry

        lax.fori_loop(0, experts, invert, 0)

    def send_blocks(target, chunk, at, peers, scaled, height=depth, sems=block_sem):
        place = (pl.ds(me * depth, height), pl.ds(at, LANES))
        waiting = None
        for peer in peers + [None]:
            if peer is not None:
                block = block_of(chunk, peer)[:height] * scaled(peer)
                sent[chunk, peer, :height] = block.astype(jnp.bfloat16)
            if waiting is not None:
                source = sent.at[chunk, waiting, pl.ds(0, height)]
                remote(source, target.at[place], sems, (ep, waiting)).start()
            waiting = peer

    def keep_block(target, chunk, at, scaled):
        sent[chunk, me] = (block_of(chunk, me) * scaled(me)).astype(jnp.bfloat16)
        place = (pl.ds(me * depth, depth), pl.ds(at, LANES))
        pltpu.make_async_copy(sent.at[chunk, me], target.at[place], own_sem).start()

    def send_stage(stage):
        for half, target in enumerate((final_gate, final_up)):
            start = max(stages[stage][0], half * groups)
            stop = min(stages[stage][1], half * groups + groups)
            ends = stop == chunks

            def send(chunk, carry, half=half, target=target):
                at = pl.multiple_of((chunk - half * groups) * LANES, LANES)
                scaled = lambda e: inverse[stage][e, pl.ds(chunk - stages[stage][0], 1), :]
                send_blocks(target, chunk, at, order, scaled)
                keep_block(target, chunk, at, scaled)
                return carry

            if start < stop:
                lax.fori_loop(start, stop - ends, send, 0)
            if ends:
                scaled = lambda e: inverse[stage][e, pl.ds(chunks - 1 - stages[stage][0], 1), :]
                send_blocks(target, chunks - 1, last, order, scaled, short, last_sem)
                keep_block(target, chunks - 1, last, scaled)

    rows[me] = (weight[...] * gain[...]).astype(jnp.bfloat16)

    wait_reads(0, 1)
    for e in range(experts):
        sums[0][pl.ds(e, 1), :] = square_sum(0, e)
    pl.semaphore_wait(barrier, len(order) + ep)
    for peer in order:
        remote(sums[0], parts[0].at[me], part_sem.at[0], (ep, peer)).start()
    parts[0][me] = sums[0][...]
    for other in others:

        @pl.when(other < ep)
        def _(other=other):
            pl.semaphore_signal(ready_sem, inc=1, device_id=(other, me), device_id_type=MESH)

    for stage in range(1, len(stages)):
        take_sums(stage)
        send_sums(stage)
        if stage == 1:
            for peer in order:
                remote(rows.at[me], rows.at[me], row_sem, (ep, peer)).start()
            for peer in order:
                source = up.at[peer, pl.ds(short, RAW), pl.ds(last, LANES)]
                remote(source, raw.at[me], raw_sem, (ep, peer)).start()

    all_of(parts[0].at[pl.ds(0, fsdp - 1)], part_sem.at[0, 1])
    total = parts[0][0]
    for s in range(1, fsdp):
        total = total + parts[0][s]
    totals[0][...] = total
    inverse[0][...] = 1.0 / jnp.sqrt(total)
    scale_gate[:, :LANES] = jnp.sqrt(totals[0][pl.ds(me, 1), :])
    scaled = lambda e: inverse[0][pl.ds(e, 1), :]

    send_blocks(final_gate, 0, 0, order[:HEAD], scaled)
    send_totals(1)
    send_blocks(final_gate, 0, 0, order[HEAD:], scaled)
    keep_block(final_gate, 0, 0, scaled)
    for stage in range(2, len(stages)):
        send_totals(stage)

    all_of(rows.at[pl.ds(0, fsdp - 1)], row_sem.at[1])

    @pl.when(ep < ep_size - 1)
    def _():
        pl.semaphore_wait(ready_sem, ep_size - 1 - ep)

    for other in others:
        remote(rows, columns.at[ep], column_sem, (other, me)).start()
    pltpu.make_async_copy(rows, columns.at[ep], small_sem).start()

    for stage in range(1, len(stages)):
        take_totals(stage)
        send_stage(stage)

    all_of(raw.at[pl.ds(0, fsdp - 1)], raw_sem.at[1])
    final = mine[pl.ds(stages[-1][1] - stages[-1][0] - 1, 1), :]
    for step in range(1, fsdp):
        source = lax.rem(me + step, fsdp)
        at = pl.multiple_of(source * depth + short, RAW)
        final_up[pl.ds(at, RAW), last : last + LANES] = (raw[source] * final).astype(jnp.bfloat16)

    pltpu.make_async_copy(rows, columns.at[ep], small_sem).wait()
    if others:
        all_of(columns.at[pl.ds(0, ep_size - 1)], column_sem.at[1])

    def turn(f, carry):
        block = columns[:, f].astype(jnp.float32).reshape(-1, depth)
        router[pl.ds(pl.multiple_of(f * depth, depth), depth), :] = block.T.astype(jnp.bfloat16)
        return carry

    lax.fori_loop(0, fsdp, turn, 0)

    for stage in range(len(stages)):
        all_of(parts[stage].at[pl.ds(0, fsdp - 1)], part_sem.at[stage, 0])
        if stage > 0:
            all_of(totals[stage].at[pl.ds(0, fsdp - 1)], total_sem.at[stage, 0])
    all_of(rows.at[pl.ds(0, fsdp - 1)], row_sem.at[0])
    if others:
        all_of(columns.at[pl.ds(0, ep_size - 1)], column_sem.at[0])
    all_of(sent.at[:, 0], own_sem)
    all_of(raw.at[pl.ds(0, fsdp - 1)], raw_sem.at[0])
    for k in range(2):
        all_of(sent.at[: chunks - 1, pl.ds(0, fsdp - 1)], block_sem.at[k])
        all_of(sent.at[chunks - 1, pl.ds(0, fsdp - 1), pl.ds(0, short)], last_sem.at[k])


def place(*refs):
    count = (len(refs) - 1) // 2
    copies = []
    for source, target in zip(refs[:count], refs[count : 2 * count]):
        pieces = 4 if source.shape[0] > 8 else 1
        step = source.shape[0] // pieces
        for k in range(pieces):
            at = pl.ds(k * step, step)
            copies.append(pltpu.make_async_copy(source.at[at], target.at[at], refs[-1].at[len(copies)]))
    for copy in copies:
        copy.start()
    for copy in copies:
        copy.wait()


def body(ep_size, fsdp, master_gate, master_up, router_weight, router_gain):
    experts, depth, width = master_gate.shape
    side = 4
    own, chunks = router_weight.shape[1], 2 * width // LANES
    stages = ((0, 1), (1, 4), (4, chunks))
    anywhere = pl.BlockSpec(memory_space=pl.ANY)
    vmem = pl.BlockSpec(memory_space=pltpu.VMEM)
    dma, pair = pltpu.SemaphoreType.DMA, pltpu.SemaphoreType.DMA((2,))

    def per_stage(lead, dtype=jnp.float32):
        return [pltpu.VMEM((lead, stop - start, LANES), dtype) for start, stop in stages[1:]]

    results = (
        ((fsdp * depth, width), jnp.bfloat16),
        ((fsdp * depth, width), jnp.bfloat16),
        ((1, width), jnp.float32),
        ((1, width), jnp.float32),
        ((fsdp * depth, ep_size * own), jnp.bfloat16),
    )
    flat = pltpu.VMEM((experts, LANES), jnp.float32)
    arrived = pl.pallas_call(
        functools.partial(kernel, ep_size, side, stages),
        out_shape=tuple(pltpu.VMEM(*result) for result in results),
        in_specs=[anywhere, anywhere, vmem, vmem],
        out_specs=[vmem] * 5,
        scratch_shapes=[
            pltpu.VMEM((2, experts, depth, width), jnp.float32),
            [flat] + per_stage(experts),
            [pltpu.VMEM((fsdp, experts, LANES), jnp.float32)] + per_stage(fsdp),
            [flat] + per_stage(experts),
            [flat] + per_stage(experts),
            pltpu.VMEM((chunks, experts, depth, LANES), jnp.bfloat16),
            pltpu.VMEM((fsdp, RAW, LANES), jnp.float32),
            pltpu.VMEM((stages[-1][1] - stages[-1][0], LANES), jnp.float32),
            pltpu.VMEM((fsdp, own, depth), jnp.bfloat16),
            pltpu.VMEM((ep_size, fsdp, own, depth), jnp.bfloat16),
            dma((4 * experts // PIECE,)), dma, dma((len(stages), 2)), dma((len(stages), 2)),
            pair, pair, pair, pair, pair, dma, pltpu.SemaphoreType.REGULAR,
        ],
        compiler_params=pltpu.CompilerParams(
            collective_id=0, has_side_effects=True, vmem_limit_bytes=48 * 2**20
        ),
        name="relayout",
    )(master_gate, master_up, router_weight.T, router_gain[None, :])
    gate, up, scale_gate, scale_up, router = pl.pallas_call(
        place,
        out_shape=tuple(jax.ShapeDtypeStruct(*result) for result in results),
        in_specs=[vmem] * 5,
        out_specs=[anywhere] * 5,
        scratch_shapes=[dma((16,))],
        compiler_params=pltpu.CompilerParams(vmem_limit_bytes=2**20),
        name="place",
    )(*(pltpu.with_memory_space_constraint(a, pltpu.VMEM) for a in arrived))
    return gate[None], up[None], scale_gate, scale_up, router


def solution(mesh):
    both = ("ep", "fsdp")
    return jax.shard_map(
        functools.partial(body, mesh.shape["ep"], mesh.shape["fsdp"]),
        mesh=mesh,
        in_specs=(P("ep", "fsdp", None), P("ep", "fsdp", None), P("fsdp", "ep"), P("fsdp")),
        out_specs=(P(both, None, None), P(both, None, None), P(both, None), P(both, None), P()),
        check_vma=False,
    )
```

```python
import functools

import jax
import jax.numpy as jnp
from jax import lax
from jax.experimental import pallas as pl
from jax.experimental.pallas import tpu as pltpu
from jax.sharding import PartitionSpec as P

MESH = pl.DeviceIdType.MESH
LANES = 128
HEAD = 3
RAW = 16
PIECE = 4
ORDER = (
    (2, 2), (2, 1), (1, 2), (2, 3), (3, 2), (1, 1), (3, 3), (1, 3),
    (3, 1), (2, 0), (0, 2), (1, 0), (0, 1), (3, 0), (0, 3),
)


def kernel(
    ep_size, side, stages, gate, up, weight, gain,
    final_gate, final_up, scale_gate, scale_up, router,
    x, sums, parts, totals, inverse, sent, raw, mine, weight_here, gain_here, rows, columns,
    in_sem, small_sem, part_sem, total_sem, raw_sem, row_sem, column_sem, block_sem, last_sem, own_sem, ready_sem, weight_sem,
):
    fsdp = side * side
    experts, depth = gate.shape[0], gate.shape[1]
    groups = gate.shape[2] // LANES
    chunks = 2 * groups
    ep, me = lax.axis_index("ep"), lax.axis_index("fsdp")
    my_z, my_y = me // side, me % side
    order = [((my_z + dz) % side) * side + (my_y + dy) % side for dy, dz in ORDER]
    others = [(ep + step) % ep_size for step in range(1, ep_size)]
    scales = (scale_gate, scale_up)
    last, short = (groups - 1) * LANES, depth - RAW

    barrier = pltpu.get_barrier_semaphore()
    reads = []
    for half, source in enumerate((gate, up)):
        for start, stop in ((0, 1), (1, 4), (4, groups)) if half == 0 else ((0, groups),):
            for e in range(0, experts, PIECE):
                part = (pl.ds(e, PIECE), slice(None), pl.ds(start * LANES, (stop - start) * LANES))
                copy = pltpu.make_async_copy(
                    source.at[part], x.at[(half, *part)], in_sem.at[len(reads)]
                )
                reads.append((half * groups + start, copy))
    for chunk, copy in reads:
        if chunk == 0:
            copy.start()
    small = (
        pltpu.make_async_copy(weight, weight_here, weight_sem.at[0]),
        pltpu.make_async_copy(gain, gain_here, weight_sem.at[1]),
    )
    for copy in small:
        copy.start()
    for peer in order:
        pl.semaphore_signal(barrier, inc=1, device_id=(ep, peer), device_id_type=MESH)
    for other in others:
        @pl.when(other > ep)
        def _(other=other):
            pl.semaphore_signal(barrier, inc=1, device_id=(other, me), device_id_type=MESH)

    for chunk, copy in reads:
        if chunk > 0:
            copy.start()

    def wait_reads(start, stop):
        for chunk, copy in reads:
            if start <= chunk < stop:
                copy.wait()

    def block_of(chunk, e):
        half = chunk // groups
        return x[half, e, :, pl.ds(pl.multiple_of((chunk - half * groups) * LANES, LANES), LANES)]

    def remote(source, target, sems, device):
        return pltpu.make_async_remote_copy(
            src_ref=source, dst_ref=target, send_sem=sems.at[0], recv_sem=sems.at[1],
            device_id=device, device_id_type=MESH,
        )

    def all_of(ref, sem):
        pltpu.make_async_copy(ref, ref, sem).wait()

    def square_sum(chunk, e):
        block = block_of(chunk, e)
        return jnp.sum(block * block, axis=0, keepdims=True)

    def take_sums(stage):
        start, stop = stages[stage]
        wait_reads(start, stop)

        def one(chunk, carry):
            for e in range(experts):
                sums[stage][e, pl.ds(chunk - start, 1), :] = square_sum(chunk, e)
            return carry

        lax.fori_loop(start, stop, one, 0)

    def send_sums(stage):
        for peer in order:
            remote(sums[stage].at[peer], parts[stage].at[me], part_sem.at[stage], (ep, peer)).start()
        parts[stage][me] = sums[stage][me]

    def send_totals(stage):
        start, stop = stages[stage]
        all_of(parts[stage].at[pl.ds(0, fsdp - 1)], part_sem.at[stage, 1])
        total = parts[stage][0]
        for s in range(1, fsdp):
            total = total + parts[stage][s]
        totals[stage][me] = total
        if stop == chunks:
            mine[...] = 1.0 / jnp.sqrt(total)
        scale = jnp.sqrt(total)
        for peer in order:
            remote(totals[stage].at[me], totals[stage].at[me], total_sem.at[stage], (ep, peer)).start()
        for chunk in range(start, stop):
            at = (chunk % groups) * LANES
            scales[chunk // groups][:, at : at + LANES] = scale[chunk - start : chunk - start + 1, :]

    def take_totals(stage):
        all_of(totals[stage].at[pl.ds(0, fsdp - 1)], total_sem.at[stage, 1])

        def invert(e, carry):
            inverse[stage][e] = 1.0 / jnp.sqrt(totals[stage][e])
            return carry

        lax.fori_loop(0, experts, invert, 0)

    def send_blocks(target, chunk, at, peers, scaled, height=depth, sems=block_sem):
        place = (pl.ds(me * depth, height), pl.ds(at, LANES))
        waiting = None
        for peer in peers + [None]:
            if peer is not None:
                block = block_of(chunk, peer)[:height] * scaled(peer)
                sent[chunk, peer, :height] = block.astype(jnp.bfloat16)
            if waiting is not None:
                source = sent.at[chunk, waiting, pl.ds(0, height)]
                remote(source, target.at[place], sems, (ep, waiting)).start()
            waiting = peer

    def keep_block(target, chunk, at, scaled):
        sent[chunk, me] = (block_of(chunk, me) * scaled(me)).astype(jnp.bfloat16)
        place = (pl.ds(me * depth, depth), pl.ds(at, LANES))
        pltpu.make_async_copy(sent.at[chunk, me], target.at[place], own_sem).start()

    def send_stage(stage):
        for half, target in enumerate((final_gate, final_up)):
            start = max(stages[stage][0], half * groups)
            stop = min(stages[stage][1], half * groups + groups)
            ends = stop == chunks

            def send(chunk, carry, half=half, target=target):
                at = pl.multiple_of((chunk - half * groups) * LANES, LANES)
                scaled = lambda e: inverse[stage][e, pl.ds(chunk - stages[stage][0], 1), :]
                send_blocks(target, chunk, at, order, scaled)
                keep_block(target, chunk, at, scaled)
                return carry

            if start < stop:
                lax.fori_loop(start, stop - ends, send, 0)
            if ends:
                scaled = lambda e: inverse[stage][e, pl.ds(chunks - 1 - stages[stage][0], 1), :]
                send_blocks(target, chunks - 1, last, order, scaled, short, last_sem)
                keep_block(target, chunks - 1, last, scaled)

    wait_reads(0, 1)
    for e in range(experts):
        sums[0][pl.ds(e, 1), :] = square_sum(0, e)
    pl.semaphore_wait(barrier, len(order) + ep)
    for peer in order:
        remote(sums[0], parts[0].at[me], part_sem.at[0], (ep, peer)).start()
    parts[0][me] = sums[0][...]
    for other in others:

        @pl.when(other < ep)
        def _(other=other):
            pl.semaphore_signal(ready_sem, inc=1, device_id=(other, me), device_id_type=MESH)

    for stage in range(1, len(stages)):
        take_sums(stage)
        send_sums(stage)
        if stage == 1:
            for copy in small:
                copy.wait()
            rows[me] = (weight_here[...] * gain_here[...]).astype(jnp.bfloat16)
            for peer in order:
                remote(rows.at[me], rows.at[me], row_sem, (ep, peer)).start()
            for peer in order:
                source = up.at[peer, pl.ds(short, RAW), pl.ds(last, LANES)]
                remote(source, raw.at[me], raw_sem, (ep, peer)).start()

    all_of(parts[0].at[pl.ds(0, fsdp - 1)], part_sem.at[0, 1])
    total = parts[0][0]
    for s in range(1, fsdp):
        total = total + parts[0][s]
    totals[0][...] = total
    inverse[0][...] = 1.0 / jnp.sqrt(total)
    scale_gate[:, :LANES] = jnp.sqrt(totals[0][pl.ds(me, 1), :])
    scaled = lambda e: inverse[0][pl.ds(e, 1), :]

    send_blocks(final_gate, 0, 0, order[:HEAD], scaled)
    send_totals(1)
    send_blocks(final_gate, 0, 0, order[HEAD:], scaled)
    keep_block(final_gate, 0, 0, scaled)
    for stage in range(2, len(stages)):
        send_totals(stage)

    all_of(rows.at[pl.ds(0, fsdp - 1)], row_sem.at[1])

    @pl.when(ep < ep_size - 1)
    def _():
        pl.semaphore_wait(ready_sem, ep_size - 1 - ep)

    for other in others:
        remote(rows, columns.at[ep], column_sem, (other, me)).start()
    pltpu.make_async_copy(rows, columns.at[ep], small_sem).start()

    for stage in range(1, len(stages)):
        take_totals(stage)
        send_stage(stage)

    all_of(raw.at[pl.ds(0, fsdp - 1)], raw_sem.at[1])
    final = mine[pl.ds(stages[-1][1] - stages[-1][0] - 1, 1), :]
    for step in range(1, fsdp):
        source = lax.rem(me + step, fsdp)
        at = pl.multiple_of(source * depth + short, RAW)
        final_up[pl.ds(at, RAW), last : last + LANES] = (raw[source] * final).astype(jnp.bfloat16)

    pltpu.make_async_copy(rows, columns.at[ep], small_sem).wait()
    if others:
        all_of(columns.at[pl.ds(0, ep_size - 1)], column_sem.at[1])

    def turn(f, carry):
        block = columns[:, f].astype(jnp.float32).reshape(-1, depth)
        router[pl.ds(pl.multiple_of(f * depth, depth), depth), :] = block.T.astype(jnp.bfloat16)
        return carry

    lax.fori_loop(0, fsdp, turn, 0)

    for stage in range(len(stages)):
        all_of(parts[stage].at[pl.ds(0, fsdp - 1)], part_sem.at[stage, 0])
        if stage > 0:
            all_of(totals[stage].at[pl.ds(0, fsdp - 1)], total_sem.at[stage, 0])
    all_of(rows.at[pl.ds(0, fsdp - 1)], row_sem.at[0])
    if others:
        all_of(columns.at[pl.ds(0, ep_size - 1)], column_sem.at[0])
    all_of(sent.at[:, 0], own_sem)
    all_of(raw.at[pl.ds(0, fsdp - 1)], raw_sem.at[0])
    for k in range(2):
        all_of(sent.at[: chunks - 1, pl.ds(0, fsdp - 1)], block_sem.at[k])
        all_of(sent.at[chunks - 1, pl.ds(0, fsdp - 1), pl.ds(0, short)], last_sem.at[k])


def place(*refs):
    count = (len(refs) - 1) // 2
    copies = []
    for source, target in zip(refs[:count], refs[count : 2 * count]):
        pieces = 4 if source.shape[0] > 8 else 1
        step = source.shape[0] // pieces
        for k in range(pieces):
            at = pl.ds(k * step, step)
            copies.append(pltpu.make_async_copy(source.at[at], target.at[at], refs[-1].at[len(copies)]))
    for copy in copies:
        copy.start()
    for copy in copies:
        copy.wait()


def body(ep_size, fsdp, master_gate, master_up, router_weight, router_gain):
    experts, depth, width = master_gate.shape
    side = 4
    own, chunks = router_weight.shape[1], 2 * width // LANES
    stages = ((0, 1), (1, 3), (3, chunks))
    anywhere = pl.BlockSpec(memory_space=pl.ANY)
    vmem = pl.BlockSpec(memory_space=pltpu.VMEM)
    dma, pair = pltpu.SemaphoreType.DMA, pltpu.SemaphoreType.DMA((2,))

    def per_stage(lead, dtype=jnp.float32):
        return [pltpu.VMEM((lead, stop - start, LANES), dtype) for start, stop in stages[1:]]

    results = (
        ((fsdp * depth, width), jnp.bfloat16),
        ((fsdp * depth, width), jnp.bfloat16),
        ((1, width), jnp.float32),
        ((1, width), jnp.float32),
        ((fsdp * depth, ep_size * own), jnp.bfloat16),
    )
    flat = pltpu.VMEM((experts, LANES), jnp.float32)
    arrived = pl.pallas_call(
        functools.partial(kernel, ep_size, side, stages),
        out_shape=tuple(pltpu.VMEM(*result) for result in results),
        in_specs=[anywhere] * 4,
        out_specs=[vmem] * 5,
        scratch_shapes=[
            pltpu.VMEM((2, experts, depth, width), jnp.float32),
            [flat] + per_stage(experts),
            [pltpu.VMEM((fsdp, experts, LANES), jnp.float32)] + per_stage(fsdp),
            [flat] + per_stage(experts),
            [flat] + per_stage(experts),
            pltpu.VMEM((chunks, experts, depth, LANES), jnp.bfloat16),
            pltpu.VMEM((fsdp, RAW, LANES), jnp.float32),
            pltpu.VMEM((stages[-1][1] - stages[-1][0], LANES), jnp.float32),
            pltpu.VMEM((own, depth), jnp.float32),
            pltpu.VMEM((1, depth), jnp.float32),
            pltpu.VMEM((fsdp, own, depth), jnp.bfloat16),
            pltpu.VMEM((ep_size, fsdp, own, depth), jnp.bfloat16),
            dma((4 * experts // PIECE,)), dma, dma((len(stages), 2)), dma((len(stages), 2)),
            pair, pair, pair, pair, pair, dma, pltpu.SemaphoreType.REGULAR, pair,
        ],
        compiler_params=pltpu.CompilerParams(
            collective_id=0, has_side_effects=True, vmem_limit_bytes=48 * 2**20
        ),
        name="relayout",
    )(master_gate, master_up, router_weight.T, router_gain[None, :])
    gate, up, scale_gate, scale_up, router = pl.pallas_call(
        place,
        out_shape=tuple(jax.ShapeDtypeStruct(*result) for result in results),
        in_specs=[vmem] * 5,
        out_specs=[anywhere] * 5,
        scratch_shapes=[dma((16,))],
        compiler_params=pltpu.CompilerParams(vmem_limit_bytes=2**20),
        name="place",
    )(*(pltpu.with_memory_space_constraint(a, pltpu.VMEM) for a in arrived))
    return gate[None], up[None], scale_gate, scale_up, router


def solution(mesh):
    both = ("ep", "fsdp")
    return jax.shard_map(
        functools.partial(body, mesh.shape["ep"], mesh.shape["fsdp"]),
        mesh=mesh,
        in_specs=(P("ep", "fsdp", None), P("ep", "fsdp", None), P("fsdp", "ep"), P("fsdp")),
        out_specs=(P(both, None, None), P(both, None, None), P(both, None), P(both, None), P()),
        check_vma=False,
    )
```

```python
import functools

import jax
import jax.numpy as jnp
from jax import lax
from jax.experimental import pallas as pl
from jax.experimental.pallas import tpu as pltpu
from jax.sharding import PartitionSpec as P

MESH = pl.DeviceIdType.MESH
LANES = 128
HEAD = 3
RAW = 16
PIECE = 8
ORDER = (
    (2, 2), (2, 1), (1, 2), (2, 3), (3, 2), (1, 1), (3, 3), (1, 3),
    (3, 1), (2, 0), (0, 2), (1, 0), (0, 1), (3, 0), (0, 3),
)


def kernel(
    ep_size, side, stages, gate, up, weight, gain,
    final_gate, final_up, scale_gate, scale_up, router,
    x, sums, parts, totals, inverse, sent, raw, mine, weight_here, gain_here, rows, columns,
    in_sem, small_sem, part_sem, total_sem, raw_sem, row_sem, column_sem, block_sem, last_sem, own_sem, ready_sem, weight_sem,
):
    fsdp = side * side
    experts, depth = gate.shape[0], gate.shape[1]
    groups = gate.shape[2] // LANES
    chunks = 2 * groups
    ep, me = lax.axis_index("ep"), lax.axis_index("fsdp")
    my_z, my_y = me // side, me % side
    order = [((my_z + dz) % side) * side + (my_y + dy) % side for dy, dz in ORDER]
    others = [(ep + step) % ep_size for step in range(1, ep_size)]
    scales = (scale_gate, scale_up)
    last, short = (groups - 1) * LANES, depth - RAW

    barrier = pltpu.get_barrier_semaphore()
    reads = []
    for half, source in enumerate((gate, up)):
        for start, stop in ((0, 1), (1, 4), (4, groups)) if half == 0 else ((0, groups),):
            for e in range(0, experts, PIECE):
                part = (pl.ds(e, PIECE), slice(None), pl.ds(start * LANES, (stop - start) * LANES))
                copy = pltpu.make_async_copy(
                    source.at[part], x.at[(half, *part)], in_sem.at[len(reads)]
                )
                reads.append((half * groups + start, copy))
    for chunk, copy in reads:
        if chunk == 0:
            copy.start()
    small = (
        pltpu.make_async_copy(weight, weight_here, weight_sem.at[0]),
        pltpu.make_async_copy(gain, gain_here, weight_sem.at[1]),
    )
    for copy in small:
        copy.start()
    for peer in order:
        pl.semaphore_signal(barrier, inc=1, device_id=(ep, peer), device_id_type=MESH)
    for other in others:
        @pl.when(other > ep)
        def _(other=other):
            pl.semaphore_signal(barrier, inc=1, device_id=(other, me), device_id_type=MESH)

    for chunk, copy in reads:
        if chunk > 0:
            copy.start()

    def wait_reads(start, stop):
        for chunk, copy in reads:
            if start <= chunk < stop:
                copy.wait()

    def block_of(chunk, e):
        half = chunk // groups
        return x[half, e, :, pl.ds(pl.multiple_of((chunk - half * groups) * LANES, LANES), LANES)]

    def remote(source, target, sems, device):
        return pltpu.make_async_remote_copy(
            src_ref=source, dst_ref=target, send_sem=sems.at[0], recv_sem=sems.at[1],
            device_id=device, device_id_type=MESH,
        )

    def all_of(ref, sem):
        pltpu.make_async_copy(ref, ref, sem).wait()

    def square_sum(chunk, e):
        block = block_of(chunk, e)
        return jnp.sum(block * block, axis=0, keepdims=True)

    def take_sums(stage):
        start, stop = stages[stage]
        wait_reads(start, stop)

        def one(chunk, carry):
            for e in range(experts):
                sums[stage][e, pl.ds(chunk - start, 1), :] = square_sum(chunk, e)
            return carry

        lax.fori_loop(start, stop, one, 0)

    def send_sums(stage):
        for peer in order:
            remote(sums[stage].at[peer], parts[stage].at[me], part_sem.at[stage], (ep, peer)).start()
        parts[stage][me] = sums[stage][me]

    def send_totals(stage):
        start, stop = stages[stage]
        all_of(parts[stage].at[pl.ds(0, fsdp - 1)], part_sem.at[stage, 1])
        total = parts[stage][0]
        for s in range(1, fsdp):
            total = total + parts[stage][s]
        totals[stage][me] = total
        if stop == chunks:
            mine[...] = 1.0 / jnp.sqrt(total)
        scale = jnp.sqrt(total)
        for peer in order:
            remote(totals[stage].at[me], totals[stage].at[me], total_sem.at[stage], (ep, peer)).start()
        for chunk in range(start, stop):
            at = (chunk % groups) * LANES
            scales[chunk // groups][:, at : at + LANES] = scale[chunk - start : chunk - start + 1, :]

    def take_totals(stage):
        all_of(totals[stage].at[pl.ds(0, fsdp - 1)], total_sem.at[stage, 1])

        def invert(e, carry):
            inverse[stage][e] = 1.0 / jnp.sqrt(totals[stage][e])
            return carry

        lax.fori_loop(0, experts, invert, 0)

    def send_blocks(target, chunk, at, peers, scaled, height=depth, sems=block_sem):
        place = (pl.ds(me * depth, height), pl.ds(at, LANES))
        waiting = None
        for peer in peers + [None]:
            if peer is not None:
                block = block_of(chunk, peer)[:height] * scaled(peer)
                sent[chunk, peer, :height] = block.astype(jnp.bfloat16)
            if waiting is not None:
                source = sent.at[chunk, waiting, pl.ds(0, height)]
                remote(source, target.at[place], sems, (ep, waiting)).start()
            waiting = peer

    def keep_block(target, chunk, at, scaled):
        sent[chunk, me] = (block_of(chunk, me) * scaled(me)).astype(jnp.bfloat16)
        place = (pl.ds(me * depth, depth), pl.ds(at, LANES))
        pltpu.make_async_copy(sent.at[chunk, me], target.at[place], own_sem).start()

    def send_stage(stage):
        for half, target in enumerate((final_gate, final_up)):
            start = max(stages[stage][0], half * groups)
            stop = min(stages[stage][1], half * groups + groups)
            ends = stop == chunks

            def send(chunk, carry, half=half, target=target):
                at = pl.multiple_of((chunk - half * groups) * LANES, LANES)
                scaled = lambda e: inverse[stage][e, pl.ds(chunk - stages[stage][0], 1), :]
                send_blocks(target, chunk, at, order, scaled)
                keep_block(target, chunk, at, scaled)
                return carry

            if start < stop:
                lax.fori_loop(start, stop - ends, send, 0)
            if ends:
                scaled = lambda e: inverse[stage][e, pl.ds(chunks - 1 - stages[stage][0], 1), :]
                send_blocks(target, chunks - 1, last, order, scaled, short, last_sem)
                keep_block(target, chunks - 1, last, scaled)

    wait_reads(0, 1)
    for e in range(experts):
        sums[0][pl.ds(e, 1), :] = square_sum(0, e)
    pl.semaphore_wait(barrier, len(order) + ep)
    for peer in order:
        remote(sums[0], parts[0].at[me], part_sem.at[0], (ep, peer)).start()
    parts[0][me] = sums[0][...]
    for other in others:

        @pl.when(other < ep)
        def _(other=other):
            pl.semaphore_signal(ready_sem, inc=1, device_id=(other, me), device_id_type=MESH)

    for stage in range(1, len(stages)):
        take_sums(stage)
        send_sums(stage)
        if stage == 1:
            for copy in small:
                copy.wait()
            rows[me] = (weight_here[...] * gain_here[...]).astype(jnp.bfloat16)
            for peer in order:
                remote(rows.at[me], rows.at[me], row_sem, (ep, peer)).start()
            for peer in order:
                source = up.at[peer, pl.ds(short, RAW), pl.ds(last, LANES)]
                remote(source, raw.at[me], raw_sem, (ep, peer)).start()

    all_of(parts[0].at[pl.ds(0, fsdp - 1)], part_sem.at[0, 1])
    total = parts[0][0]
    for s in range(1, fsdp):
        total = total + parts[0][s]
    totals[0][...] = total
    inverse[0][...] = 1.0 / jnp.sqrt(total)
    scale_gate[:, :LANES] = jnp.sqrt(totals[0][pl.ds(me, 1), :])
    scaled = lambda e: inverse[0][pl.ds(e, 1), :]

    send_blocks(final_gate, 0, 0, order[:HEAD], scaled)
    send_totals(1)
    send_blocks(final_gate, 0, 0, order[HEAD:], scaled)
    keep_block(final_gate, 0, 0, scaled)
    for stage in range(2, len(stages)):
        send_totals(stage)

    all_of(rows.at[pl.ds(0, fsdp - 1)], row_sem.at[1])

    @pl.when(ep < ep_size - 1)
    def _():
        pl.semaphore_wait(ready_sem, ep_size - 1 - ep)

    for other in others:
        remote(rows, columns.at[ep], column_sem, (other, me)).start()
    pltpu.make_async_copy(rows, columns.at[ep], small_sem).start()

    for stage in range(1, len(stages)):
        take_totals(stage)
        send_stage(stage)

    all_of(raw.at[pl.ds(0, fsdp - 1)], raw_sem.at[1])
    final = mine[pl.ds(stages[-1][1] - stages[-1][0] - 1, 1), :]
    for step in range(1, fsdp):
        source = lax.rem(me + step, fsdp)
        at = pl.multiple_of(source * depth + short, RAW)
        final_up[pl.ds(at, RAW), last : last + LANES] = (raw[source] * final).astype(jnp.bfloat16)

    pltpu.make_async_copy(rows, columns.at[ep], small_sem).wait()
    if others:
        all_of(columns.at[pl.ds(0, ep_size - 1)], column_sem.at[1])

    def turn(f, carry):
        block = columns[:, f].astype(jnp.float32).reshape(-1, depth)
        router[pl.ds(pl.multiple_of(f * depth, depth), depth), :] = block.T.astype(jnp.bfloat16)
        return carry

    lax.fori_loop(0, fsdp, turn, 0)

    for stage in range(len(stages)):
        all_of(parts[stage].at[pl.ds(0, fsdp - 1)], part_sem.at[stage, 0])
        if stage > 0:
            all_of(totals[stage].at[pl.ds(0, fsdp - 1)], total_sem.at[stage, 0])
    all_of(rows.at[pl.ds(0, fsdp - 1)], row_sem.at[0])
    if others:
        all_of(columns.at[pl.ds(0, ep_size - 1)], column_sem.at[0])
    all_of(sent.at[:, 0], own_sem)
    all_of(raw.at[pl.ds(0, fsdp - 1)], raw_sem.at[0])
    for k in range(2):
        all_of(sent.at[: chunks - 1, pl.ds(0, fsdp - 1)], block_sem.at[k])
        all_of(sent.at[chunks - 1, pl.ds(0, fsdp - 1), pl.ds(0, short)], last_sem.at[k])


def place(*refs):
    count = (len(refs) - 1) // 2
    copies = []
    for source, target in zip(refs[:count], refs[count : 2 * count]):
        pieces = 1
        step = source.shape[0] // pieces
        for k in range(pieces):
            at = pl.ds(k * step, step)
            copies.append(pltpu.make_async_copy(source.at[at], target.at[at], refs[-1].at[len(copies)]))
    for copy in copies:
        copy.start()
    for copy in copies:
        copy.wait()


def body(ep_size, fsdp, master_gate, master_up, router_weight, router_gain):
    experts, depth, width = master_gate.shape
    side = 4
    own, chunks = router_weight.shape[1], 2 * width // LANES
    stages = ((0, 1), (1, 3), (3, chunks))
    anywhere = pl.BlockSpec(memory_space=pl.ANY)
    vmem = pl.BlockSpec(memory_space=pltpu.VMEM)
    dma, pair = pltpu.SemaphoreType.DMA, pltpu.SemaphoreType.DMA((2,))

    def per_stage(lead, dtype=jnp.float32):
        return [pltpu.VMEM((lead, stop - start, LANES), dtype) for start, stop in stages[1:]]

    results = (
        ((fsdp * depth, width), jnp.bfloat16),
        ((fsdp * depth, width), jnp.bfloat16),
        ((1, width), jnp.float32),
        ((1, width), jnp.float32),
        ((fsdp * depth, ep_size * own), jnp.bfloat16),
    )
    flat = pltpu.VMEM((experts, LANES), jnp.float32)
    arrived = pl.pallas_call(
        functools.partial(kernel, ep_size, side, stages),
        out_shape=tuple(pltpu.VMEM(*result) for result in results),
        in_specs=[anywhere] * 4,
        out_specs=[vmem] * 5,
        scratch_shapes=[
            pltpu.VMEM((2, experts, depth, width), jnp.float32),
            [flat] + per_stage(experts),
            [pltpu.VMEM((fsdp, experts, LANES), jnp.float32)] + per_stage(fsdp),
            [flat] + per_stage(experts),
            [flat] + per_stage(experts),
            pltpu.VMEM((chunks, experts, depth, LANES), jnp.bfloat16),
            pltpu.VMEM((fsdp, RAW, LANES), jnp.float32),
            pltpu.VMEM((stages[-1][1] - stages[-1][0], LANES), jnp.float32),
            pltpu.VMEM((own, depth), jnp.float32),
            pltpu.VMEM((1, depth), jnp.float32),
            pltpu.VMEM((fsdp, own, depth), jnp.bfloat16),
            pltpu.VMEM((ep_size, fsdp, own, depth), jnp.bfloat16),
            dma((4 * experts // PIECE,)), dma, dma((len(stages), 2)), dma((len(stages), 2)),
            pair, pair, pair, pair, pair, dma, pltpu.SemaphoreType.REGULAR, pair,
        ],
        compiler_params=pltpu.CompilerParams(
            collective_id=0, has_side_effects=True, vmem_limit_bytes=48 * 2**20
        ),
        name="relayout",
    )(master_gate, master_up, router_weight.T, router_gain[None, :])
    gate, up, scale_gate, scale_up, router = pl.pallas_call(
        place,
        out_shape=tuple(jax.ShapeDtypeStruct(*result) for result in results),
        in_specs=[vmem] * 5,
        out_specs=[anywhere] * 5,
        scratch_shapes=[dma((16,))],
        compiler_params=pltpu.CompilerParams(vmem_limit_bytes=2**20),
        name="place",
    )(*(pltpu.with_memory_space_constraint(a, pltpu.VMEM) for a in arrived))
    return gate[None], up[None], scale_gate, scale_up, router


def solution(mesh):
    both = ("ep", "fsdp")
    return jax.shard_map(
        functools.partial(body, mesh.shape["ep"], mesh.shape["fsdp"]),
        mesh=mesh,
        in_specs=(P("ep", "fsdp", None), P("ep", "fsdp", None), P("fsdp", "ep"), P("fsdp")),
        out_specs=(P(both, None, None), P(both, None, None), P(both, None), P(both, None), P()),
        check_vma=False,
    )
```

```python
import functools

import jax
import jax.numpy as jnp
from jax import lax
from jax.experimental import pallas as pl
from jax.experimental.pallas import tpu as pltpu
from jax.sharding import PartitionSpec as P

MESH = pl.DeviceIdType.MESH
LANES = 128
HEAD = 3
RAW = 16
PIECE = 4
ORDER = (
    (2, 2), (2, 1), (1, 2), (2, 3), (3, 2), (1, 1), (3, 3), (1, 3),
    (3, 1), (2, 0), (0, 2), (1, 0), (0, 1), (3, 0), (0, 3),
)


def kernel(
    ep_size, side, stages, gate, up, weight, gain,
    final_gate, final_up, scale_gate, scale_up, router,
    x, sums, parts, totals, inverse, sent, raw, mine, weight_here, gain_here, rows, columns,
    in_sem, small_sem, part_sem, total_sem, raw_sem, row_sem, column_sem, block_sem, last_sem, own_sem, ready_sem, weight_sem,
):
    fsdp = side * side
    experts, depth = gate.shape[0], gate.shape[1]
    groups = gate.shape[2] // LANES
    chunks = 2 * groups
    ep, me = lax.axis_index("ep"), lax.axis_index("fsdp")
    my_z, my_y = me // side, me % side
    order = [((my_z + dz) % side) * side + (my_y + dy) % side for dy, dz in ORDER]
    others = [(ep + step) % ep_size for step in range(1, ep_size)]
    scales = (scale_gate, scale_up)
    last, short = (groups - 1) * LANES, depth - RAW

    barrier = pltpu.get_barrier_semaphore()
    reads = []
    for half, source in enumerate((gate, up)):
        for start, stop in ((0, 1), (1, 4), (4, groups)) if half == 0 else ((0, groups),):
            for e in range(0, experts, PIECE):
                part = (pl.ds(e, PIECE), slice(None), pl.ds(start * LANES, (stop - start) * LANES))
                copy = pltpu.make_async_copy(
                    source.at[part], x.at[(half, *part)], in_sem.at[len(reads)]
                )
                reads.append((half * groups + start, copy))
    for chunk, copy in reads:
        if chunk == 0:
            copy.start()
    small = (
        pltpu.make_async_copy(weight, weight_here, weight_sem.at[0]),
        pltpu.make_async_copy(gain, gain_here, weight_sem.at[1]),
    )
    for copy in small:
        copy.start()
    for peer in order:
        pl.semaphore_signal(barrier, inc=1, device_id=(ep, peer), device_id_type=MESH)
    for other in others:
        @pl.when(other > ep)
        def _(other=other):
            pl.semaphore_signal(barrier, inc=1, device_id=(other, me), device_id_type=MESH)

    for chunk, copy in reads:
        if chunk > 0:
            copy.start()

    def wait_reads(start, stop):
        for chunk, copy in reads:
            if start <= chunk < stop:
                copy.wait()

    def block_of(chunk, e):
        half = chunk // groups
        return x[half, e, :, pl.ds(pl.multiple_of((chunk - half * groups) * LANES, LANES), LANES)]

    def remote(source, target, sems, device):
        return pltpu.make_async_remote_copy(
            src_ref=source, dst_ref=target, send_sem=sems.at[0], recv_sem=sems.at[1],
            device_id=device, device_id_type=MESH,
        )

    def all_of(ref, sem):
        pltpu.make_async_copy(ref, ref, sem).wait()

    def square_sum(chunk, e):
        block = block_of(chunk, e)
        return jnp.sum(block * block, axis=0, keepdims=True)

    def take_sums(stage):
        start, stop = stages[stage]
        wait_reads(start, stop)

        def one(chunk, carry):
            for e in range(experts):
                sums[stage][e, pl.ds(chunk - start, 1), :] = square_sum(chunk, e)
            return carry

        lax.fori_loop(start, stop, one, 0)

    def send_sums(stage):
        for peer in order:
            remote(sums[stage].at[peer], parts[stage].at[me], part_sem.at[stage], (ep, peer)).start()
        parts[stage][me] = sums[stage][me]

    def send_totals(stage):
        start, stop = stages[stage]
        all_of(parts[stage].at[pl.ds(0, fsdp - 1)], part_sem.at[stage, 1])
        total = parts[stage][0]
        for s in range(1, fsdp):
            total = total + parts[stage][s]
        totals[stage][me] = total
        if stop == chunks:
            mine[...] = 1.0 / jnp.sqrt(total)
        scale = jnp.sqrt(total)
        for peer in order:
            remote(totals[stage].at[me], totals[stage].at[me], total_sem.at[stage], (ep, peer)).start()
        for chunk in range(start, stop):
            at = (chunk % groups) * LANES
            scales[chunk // groups][:, at : at + LANES] = scale[chunk - start : chunk - start + 1, :]

    def take_totals(stage):
        all_of(totals[stage].at[pl.ds(0, fsdp - 1)], total_sem.at[stage, 1])

        def invert(e, carry):
            inverse[stage][e] = 1.0 / jnp.sqrt(totals[stage][e])
            return carry

        lax.fori_loop(0, experts, invert, 0)

    def send_blocks(target, chunk, at, peers, scaled, height=depth, sems=block_sem):
        place = (pl.ds(me * depth, height), pl.ds(at, LANES))
        waiting = None
        for peer in peers + [None]:
            if peer is not None:
                block = block_of(chunk, peer)[:height] * scaled(peer)
                sent[chunk, peer, :height] = block.astype(jnp.bfloat16)
            if waiting is not None:
                source = sent.at[chunk, waiting, pl.ds(0, height)]
                remote(source, target.at[place], sems, (ep, waiting)).start()
            waiting = peer

    def keep_block(target, chunk, at, scaled):
        sent[chunk, me] = (block_of(chunk, me) * scaled(me)).astype(jnp.bfloat16)
        place = (pl.ds(me * depth, depth), pl.ds(at, LANES))
        pltpu.make_async_copy(sent.at[chunk, me], target.at[place], own_sem).start()

    def send_stage(stage):
        for half, target in enumerate((final_gate, final_up)):
            start = max(stages[stage][0], half * groups)
            stop = min(stages[stage][1], half * groups + groups)
            ends = stop == chunks

            def send(chunk, carry, half=half, target=target):
                at = pl.multiple_of((chunk - half * groups) * LANES, LANES)
                scaled = lambda e: inverse[stage][e, pl.ds(chunk - stages[stage][0], 1), :]
                send_blocks(target, chunk, at, order, scaled)
                keep_block(target, chunk, at, scaled)
                return carry

            if start < stop:
                lax.fori_loop(start, stop - ends, send, 0)
            if ends:
                scaled = lambda e: inverse[stage][e, pl.ds(chunks - 1 - stages[stage][0], 1), :]
                send_blocks(target, chunks - 1, last, order, scaled, short, last_sem)
                keep_block(target, chunks - 1, last, scaled)

    wait_reads(0, 1)
    for e in range(experts):
        sums[0][pl.ds(e, 1), :] = square_sum(0, e)
    pl.semaphore_wait(barrier, len(order) + ep)
    for peer in order:
        remote(sums[0], parts[0].at[me], part_sem.at[0], (ep, peer)).start()
    parts[0][me] = sums[0][...]
    for other in others:

        @pl.when(other < ep)
        def _(other=other):
            pl.semaphore_signal(ready_sem, inc=1, device_id=(other, me), device_id_type=MESH)

    for stage in range(1, len(stages)):
        take_sums(stage)
        send_sums(stage)
        if stage == 1:
            for copy in small:
                copy.wait()
            rows[me] = (weight_here[...] * gain_here[...]).astype(jnp.bfloat16)
            for peer in order:
                remote(rows.at[me], rows.at[me], row_sem, (ep, peer)).start()
            for peer in order:
                source = up.at[peer, pl.ds(short, RAW), pl.ds(last, LANES)]
                remote(source, raw.at[me], raw_sem, (ep, peer)).start()

    all_of(parts[0].at[pl.ds(0, fsdp - 1)], part_sem.at[0, 1])
    total = parts[0][0]
    for s in range(1, fsdp):
        total = total + parts[0][s]
    totals[0][...] = total
    inverse[0][...] = 1.0 / jnp.sqrt(total)
    scale_gate[:, :LANES] = jnp.sqrt(totals[0][pl.ds(me, 1), :])
    scaled = lambda e: inverse[0][pl.ds(e, 1), :]

    send_blocks(final_gate, 0, 0, order[:HEAD], scaled)
    send_totals(1)
    send_blocks(final_gate, 0, 0, order[HEAD:], scaled)
    keep_block(final_gate, 0, 0, scaled)
    for stage in range(2, len(stages)):
        send_totals(stage)

    all_of(rows.at[pl.ds(0, fsdp - 1)], row_sem.at[1])

    @pl.when(ep < ep_size - 1)
    def _():
        pl.semaphore_wait(ready_sem, ep_size - 1 - ep)

    for other in others:
        remote(rows, columns.at[ep], column_sem, (other, me)).start()
    pltpu.make_async_copy(rows, columns.at[ep], small_sem).start()

    for stage in range(1, len(stages)):
        take_totals(stage)
        send_stage(stage)

    all_of(raw.at[pl.ds(0, fsdp - 1)], raw_sem.at[1])
    final = mine[pl.ds(stages[-1][1] - stages[-1][0] - 1, 1), :]
    for step in range(1, fsdp):
        source = lax.rem(me + step, fsdp)
        at = pl.multiple_of(source * depth + short, RAW)
        final_up[pl.ds(at, RAW), last : last + LANES] = (raw[source] * final).astype(jnp.bfloat16)

    pltpu.make_async_copy(rows, columns.at[ep], small_sem).wait()
    if others:
        all_of(columns.at[pl.ds(0, ep_size - 1)], column_sem.at[1])

    def turn(f, carry):
        block = columns[:, f].astype(jnp.float32).reshape(-1, depth)
        router[pl.ds(pl.multiple_of(f * depth, depth), depth), :] = block.T.astype(jnp.bfloat16)
        return carry

    lax.fori_loop(0, fsdp, turn, 0)

    for stage in range(len(stages)):
        all_of(parts[stage].at[pl.ds(0, fsdp - 1)], part_sem.at[stage, 0])
        if stage > 0:
            all_of(totals[stage].at[pl.ds(0, fsdp - 1)], total_sem.at[stage, 0])
    all_of(rows.at[pl.ds(0, fsdp - 1)], row_sem.at[0])
    if others:
        all_of(columns.at[pl.ds(0, ep_size - 1)], column_sem.at[0])
    all_of(sent.at[:, 0], own_sem)
    all_of(raw.at[pl.ds(0, fsdp - 1)], raw_sem.at[0])
    for k in range(2):
        all_of(sent.at[: chunks - 1, pl.ds(0, fsdp - 1)], block_sem.at[k])
        all_of(sent.at[chunks - 1, pl.ds(0, fsdp - 1), pl.ds(0, short)], last_sem.at[k])


def place(*refs):
    count = (len(refs) - 1) // 2
    copies = []
    for source, target in zip(refs[:count], refs[count : 2 * count]):
        pieces = 4 if source.shape[0] > 8 else 1
        step = source.shape[0] // pieces
        for k in range(pieces):
            at = pl.ds(k * step, step)
            copies.append(pltpu.make_async_copy(source.at[at], target.at[at], refs[-1].at[len(copies)]))
    for copy in copies:
        copy.start()
    for copy in copies:
        copy.wait()


def body(ep_size, fsdp, master_gate, master_up, router_weight, router_gain):
    experts, depth, width = master_gate.shape
    side = 4
    own, chunks = router_weight.shape[1], 2 * width // LANES
    stages = ((0, 1), (1, 4), (4, chunks))
    anywhere = pl.BlockSpec(memory_space=pl.ANY)
    vmem = pl.BlockSpec(memory_space=pltpu.VMEM)
    dma, pair = pltpu.SemaphoreType.DMA, pltpu.SemaphoreType.DMA((2,))

    def per_stage(lead, dtype=jnp.float32):
        return [pltpu.VMEM((lead, stop - start, LANES), dtype) for start, stop in stages[1:]]

    results = (
        ((fsdp * depth, width), jnp.bfloat16),
        ((fsdp * depth, width), jnp.bfloat16),
        ((1, width), jnp.float32),
        ((1, width), jnp.float32),
        ((fsdp * depth, ep_size * own), jnp.bfloat16),
    )
    flat = pltpu.VMEM((experts, LANES), jnp.float32)
    arrived = pl.pallas_call(
        functools.partial(kernel, ep_size, side, stages),
        out_shape=tuple(pltpu.VMEM(*result) for result in results),
        in_specs=[anywhere] * 4,
        out_specs=[vmem] * 5,
        scratch_shapes=[
            pltpu.VMEM((2, experts, depth, width), jnp.float32),
            [flat] + per_stage(experts),
            [pltpu.VMEM((fsdp, experts, LANES), jnp.float32)] + per_stage(fsdp),
            [flat] + per_stage(experts),
            [flat] + per_stage(experts),
            pltpu.VMEM((chunks, experts, depth, LANES), jnp.bfloat16),
            pltpu.VMEM((fsdp, RAW, LANES), jnp.float32),
            pltpu.VMEM((stages[-1][1] - stages[-1][0], LANES), jnp.float32),
            pltpu.VMEM((own, depth), jnp.float32),
            pltpu.VMEM((1, depth), jnp.float32),
            pltpu.VMEM((fsdp, own, depth), jnp.bfloat16),
            pltpu.VMEM((ep_size, fsdp, own, depth), jnp.bfloat16),
            dma((4 * experts // PIECE,)), dma, dma((len(stages), 2)), dma((len(stages), 2)),
            pair, pair, pair, pair, pair, dma, pltpu.SemaphoreType.REGULAR, pair,
        ],
        compiler_params=pltpu.CompilerParams(
            collective_id=0, has_side_effects=True, vmem_limit_bytes=48 * 2**20
        ),
        name="relayout",
    )(master_gate, master_up, router_weight.T, router_gain[None, :])
    gate, up, scale_gate, scale_up, router = pl.pallas_call(
        place,
        out_shape=tuple(jax.ShapeDtypeStruct(*result) for result in results),
        in_specs=[vmem] * 5,
        out_specs=[anywhere] * 5,
        scratch_shapes=[dma((16,))],
        compiler_params=pltpu.CompilerParams(vmem_limit_bytes=2**20),
        name="place",
    )(*(pltpu.with_memory_space_constraint(a, pltpu.VMEM) for a in arrived))
    return gate[None], up[None], scale_gate, scale_up, router


def solution(mesh):
    both = ("ep", "fsdp")
    return jax.shard_map(
        functools.partial(body, mesh.shape["ep"], mesh.shape["fsdp"]),
        mesh=mesh,
        in_specs=(P("ep", "fsdp", None), P("ep", "fsdp", None), P("fsdp", "ep"), P("fsdp")),
        out_specs=(P(both, None, None), P(both, None, None), P(both, None), P(both, None), P()),
        check_vma=False,
    )
```
